32 devices in a mesh: tok: 4 (over y, x), col: 8 (over z, core).
Axes of the slice: x: 2, y: 2, z: 4, core: 2. Of those that a mesh axis runs over, the one named last changes fastest.
Arguments:
- row_bank: bfloat16 [16384, 8192], P(None, 'col'), may hold values from -50 to 50
- token_ids: int32 [6144], P('tok'), may hold values from 0 to 16383
- sign_flips: int32 [8192], P('col'), may hold values from -1 to 1, as said below
- damping: float32 [1], replicated, may hold values from 0.1 to 1
Outputs:
- hessian: float32 [8192, 8192], P('tok', 'col')
The draws below stay inside these ranges and needn't reach their ends.
Inputs may be any that keep to these rules, and one draw needn't show every extreme that they name: `sign_flips`: each entry is -1 or 1.
All inputs are finite; a program needn't handle non-finite values.
Results may differ from the reference program's by a relative error of at most 0.0003.
The reference program's roundings to bfloat16 on the way (of `picked`, `half_turned` and `rotated`) count: a program that leaves them out, or rounds other values in their place, can miss the bound.
Values may be sent and summed in bfloat16 or wider, within the bound.
A program may use at most 192 MiB of HBM per device.

```python
import math
import jax
import jax.numpy as jnp

D = 8192
BLOCK = 32
TOKENS = 6144
BANK = 16384


def draw_sign_flips(key, part):
    return 2 * jax.random.randint(key, (D,), 0, 2, dtype=jnp.int32) - 1


def draw_token_ids(key, part):
    spot = jnp.arange(TOKENS, dtype=jnp.int32)
    start = spot * (BANK // 2) // TOKENS
    jitter = jax.random.randint(jax.random.fold_in(key, 11), (TOKENS,), 0, BANK // 2, dtype=jnp.int32)
    return start + jitter


def draw_row_bank(key, part):
    place = jnp.arange(BANK, dtype=jnp.float32) / BANK
    lift = jax.random.uniform(jax.random.fold_in(key, 21), (BANK,), jnp.float32)
    row_scale = jnp.power(10.0, 0.8 * place + 0.4 * lift)
    col_scale = jnp.exp(jax.random.uniform(jax.random.fold_in(key, 22), (D,), jnp.float32) * math.log(10.0))
    noise = jnp.clip(jax.random.normal(jax.random.fold_in(key, 23), (BANK, D), jnp.float32), -6.0, 6.0)
    values = noise * row_scale[:, None] * col_scale[None, :] / 30.0
    return values.astype(jnp.bfloat16)


def setup_inputs(seed: int = 0) -> dict:
    key_list = jax.random.split(jax.random.key(seed), 5)
    row_bank = draw_row_bank(jax.random.fold_in(key_list[4], 71), 0)
    token_ids = draw_token_ids(jax.random.fold_in(key_list[4], 71), 0)
    sign_flips = draw_sign_flips(jax.random.fold_in(key_list[4], 71), 0)
    damping = jnp.clip(jnp.exp(jax.random.uniform(key_list[3], (1,), jnp.float32, math.log(0.1), math.log(1.0))), 0.1, 1.0)
    return dict(row_bank=row_bank, token_ids=token_ids, sign_flips=sign_flips, damping=damping)


def hadamard(order):
    index_range = jnp.arange(order, dtype=jnp.int32)
    anded = jnp.bitwise_and(index_range[:, None], index_range[None, :])
    parity = jnp.zeros((order, order), jnp.int32)
    for bit_place in range(int(order).bit_length()):
        parity = parity + jnp.bitwise_and(jnp.right_shift(anded, bit_place), 1)
    return (1 - 2 * jnp.bitwise_and(parity, 1)).astype(jnp.float32)

def reference(row_bank, token_ids, sign_flips, damping):
    groups = D // BLOCK
    picked = row_bank[token_ids] * sign_flips.astype(jnp.bfloat16)[None, :]
    grouped_rows = picked.reshape(TOKENS, groups, BLOCK).astype(jnp.float32)
    half_turned = jnp.einsum('rab,bc->rac', grouped_rows, hadamard(BLOCK)).astype(jnp.bfloat16)
    turned = jnp.einsum('rab,ac->rcb', half_turned.astype(jnp.float32), hadamard(groups)) * (1.0 / math.sqrt(D))
    rotated = turned.astype(jnp.bfloat16).reshape(TOKENS, D)
    gram_matrix = jnp.dot(rotated.T, rotated, preferred_element_type=jnp.float32) / TOKENS
    mean_diag = jnp.mean(jnp.diagonal(gram_matrix))
    return gram_matrix + damping[0] * mean_diag * jnp.eye(D, dtype=jnp.float32)
```

```python
import functools
import math

import jax
import jax.numpy as jnp
import numpy as np
from jax import lax
from jax.experimental import pallas as pl
from jax.experimental.pallas import tpu as pltpu
from jax.sharding import PartitionSpec as P

D = 8192
BLOCK = 32
LANES = 512
MESH = pl.DeviceIdType.MESH


def hadamard(order):
    index_range = jnp.arange(order, dtype=jnp.int32)
    anded = jnp.bitwise_and(index_range[:, None], index_range[None, :])
    parity = jnp.zeros((order, order), jnp.int32)
    for bit_place in range(int(order).bit_length()):
        parity = parity + jnp.bitwise_and(jnp.right_shift(anded, bit_place), 1)
    return (1 - 2 * jnp.bitwise_and(parity, 1)).astype(jnp.bfloat16)


def sylvester(order):
    table = np.ones((1, 1))
    while table.shape[0] < order:
        table = np.block([[table, table], [table, -table]])
    return table


def fused_kernel(
    planes, chunks, rows, piece, slots, scale,
    half_ref, table_ref,
    gram_ref, square_ref, full_ref, hop_ref,
    xbuf, tmp, rot, rxr, rxq, rxm, acc, squares,
    part_send, part_recv, z_send, z_recv, r_send, r_recv, q_send, q_recv,
    h_send, h_recv, m_send, m_recv, s_send, s_recv, load_sem, out_sem,
):
    tok = lax.axis_index("tok")
    col = lax.axis_index("col")
    plane, core = col // 2, col % 2
    mate = plane * 2 + (1 - core)
    ypos, xpos = tok // 2, tok % 2
    peers = {1: ypos * 2 + (1 - xpos), 2: (1 - ypos) * 2 + xpos, 3: 3 - tok}
    wide = 2 * piece
    role = ((ypos + plane // 2) % 2) * 2 + (xpos + plane) % 2

    barrier = pltpu.get_barrier_semaphore()
    greet = [(tok, mate)]
    for m in (1, 2, 3):
        greet.append((peers[m], col))
        greet.append((peers[m], mate))
    for m in range(1, planes):
        greet.append((tok, ((plane + m) % planes) * 2 + core))
    for device in greet:
        pl.semaphore_signal(barrier, inc=1, device_id=device, device_id_type=MESH)
    pl.semaphore_wait(barrier, len(greet))

    def part_copy(k):
        return pltpu.make_async_remote_copy(
            src_ref=half_ref.at[1 - core, k], dst_ref=full_ref.at[k, col],
            send_sem=part_send.at[k], recv_sem=part_recv.at[k],
            device_id=(tok, mate), device_id_type=MESH)

    def part_arrival(k):
        return pltpu.make_async_remote_copy(
            src_ref=half_ref.at[1 - core, k], dst_ref=full_ref.at[k, mate],
            send_sem=part_send.at[k], recv_sem=part_recv.at[k],
            device_id=(tok, mate), device_id_type=MESH)

    def z_copy(k, j, way, own=False):
        source = half_ref.at[core, k] if own else full_ref.at[k, j]
        return pltpu.make_async_remote_copy(
            src_ref=source, dst_ref=full_ref.at[k, j],
            send_sem=z_send.at[k, j, way], recv_sem=z_recv.at[k, j],
            device_id=(tok, col + 2 - 4 * way), device_id_type=MESH)

    can = {0: plane < planes - 1, 1: plane > 0}

    def own_sends(k):
        for way in (0, 1):
            @pl.when(can[way])
            def _():
                z_copy(k, col, way, own=True).start()
        part_arrival(k).wait_recv()
        for way in (0, 1):
            @pl.when(can[way])
            def _():
                z_copy(k, mate, way).start()

    def z_stage(k, distance):
        for way, origin in ((0, plane - distance), (1, plane + distance)):
            @pl.when((origin >= 0) & (origin < planes))
            def _():
                for side in (0, 1):
                    j = origin * 2 + (core if side == 0 else 1 - core)
                    z_copy(k, j, way).wait_recv()

                    @pl.when(can[way])
                    def _():
                        z_copy(k, j, way).start()

    def col_copy(k, m):
        return pltpu.make_async_remote_copy(
            src_ref=rot.at[k % slots, pl.ds(plane * wide, wide)],
            dst_ref=rxq.at[k, :, pl.ds(m * rows, rows)],
            send_sem=q_send.at[k, m], recv_sem=q_recv.at[k, m],
            device_id=(peers[m], col), device_id_type=MESH)

    def relay_copy(k, m):
        return pltpu.make_async_remote_copy(
            src_ref=rxq.at[k, :, pl.ds(m * rows, rows)],
            dst_ref=rxq.at[k, :, pl.ds(3 * rows, rows)],
            send_sem=q_send.at[k, 2 + m], recv_sem=q_recv.at[k, 3],
            device_id=(peers[3 - m], col), device_id_type=MESH)

    def row_copy(k, m):
        return pltpu.make_async_remote_copy(
            src_ref=rot.at[k % slots, pl.ds(peers[m] * wide, wide)],
            dst_ref=rxr.at[k, :, pl.ds(m * rows, rows)],
            send_sem=r_send.at[k, m], recv_sem=r_recv.at[k, m],
            device_id=(peers[m], col), device_id_type=MESH)

    def hop_copy(k, m):
        return pltpu.make_async_remote_copy(
            src_ref=rot.at[k % slots, pl.ds(peers[3] * wide, wide)],
            dst_ref=hop_ref.at[m - 1, k],
            send_sem=r_send.at[k, 3], recv_sem=h_recv.at[k, m],
            device_id=(peers[m], col), device_id_type=MESH)

    def hop_forward(k, m):
        return pltpu.make_async_remote_copy(
            src_ref=hop_ref.at[m - 1, k],
            dst_ref=rxr.at[k, :, pl.ds(3 * rows, rows)],
            send_sem=h_send.at[k, m], recv_sem=r_recv.at[k, 3],
            device_id=(peers[3 - m], col), device_id_type=MESH)

    def turn(k):
        return (k + 2 * core) % 4

    def y_first(k, sender):
        phase = turn(k)
        return (
            ((sender == 0) & (phase % 2 == 0))
            | ((sender == 2) & (phase < 3))
            | ((sender == 1) & (phase == 0))
        )

    def hops_here(k, m):
        if m == 2:
            return y_first(k, (role + 2) % 4)
        sender = role + 1 - 2 * (role % 2)
        return (sender != 3) & jnp.logical_not(y_first(k, sender))

    def relays_here(k, m):
        even = turn(k) % 2 == 0
        if m == 1:
            return (role >= 2) | ((role == 1) & even)
        return (role == 3) | ((role == 2) & (turn(k) % 2 == 1))

    def send_chunk(k):
        for m in (1, 2):
            col_copy(k, m).start()
        hop = y_first(k, role)

        @pl.when(hop)
        def _():
            hop_copy(k, 2).start()

        @pl.when(jnp.logical_not(hop) & (role != 3))
        def _():
            hop_copy(k, 1).start()

        for m in (1, 2):
            @pl.when(role != m)
            def _():
                row_copy(k, m).start()

    def sent_chunk(k):
        for m in (1, 2):
            col_copy(k, m).wait_send()
        for m in (1, 2, 3):
            @pl.when(role != m)
            def _():
                row_copy(k, m).wait_send()

    def relay(k):
        for m in (1, 2):
            col_copy(k, m).wait_recv()

            @pl.when(relays_here(k, m))
            def _():
                relay_copy(k, m).start()

        for m in (1, 2):
            @pl.when(hops_here(k, m))
            def _():
                hop_copy(k, m).wait_recv()
                hop_forward(k, m).start()

    def pass_rows(k, same):
        source = rxq.at[k] if same else rxr.at[k, :, pl.ds(0, 4 * rows)]
        return pltpu.make_async_remote_copy(
            src_ref=source, dst_ref=rxr.at[k, :, pl.ds(4 * rows, 4 * rows)],
            send_sem=m_send.at[k, 0], recv_sem=m_recv.at[k, 0],
            device_id=(tok, mate), device_id_type=MESH)

    def pass_cols(k):
        return pltpu.make_async_remote_copy(
            src_ref=rxq.at[k, pl.ds((1 - core) * piece, piece)], dst_ref=rxm.at[k],
            send_sem=m_send.at[k, 1], recv_sem=m_recv.at[k, 1],
            device_id=(tok, mate), device_id_type=MESH)

    def arrivals(k):
        relay_copy(k, 1).wait_recv()
        pass_cols(k).start()

        @pl.when(role != 0)
        def _():
            for m in (1, 2, 3):
                row_copy(k, m).wait_recv()
            pass_rows(k, False).start()

        @pl.when(role == 0)
        def _():
            pass_rows(k, True).start()
            for f in range(wide):
                rxr[k, f, pl.ds(0, 4 * rows)] = rxq[k, f]

    def loads(k):
        copies = [pltpu.make_async_copy(half_ref.at[core, k], xbuf.at[col], load_sem.at[0])]
        copies.append(pltpu.make_async_copy(full_ref.at[k, mate], xbuf.at[mate], load_sem.at[1]))
        for m in range(1, planes):
            other = ((plane + m) % planes) * 2
            copies.append(pltpu.make_async_copy(
                full_ref.at[k, pl.ds(other, 2)], xbuf.at[pl.ds(other, 2)], load_sem.at[1 + m]))
        return copies

    groups = 2 * planes * piece

    def rotate(k):
        slot = k % slots

        def product(j, carry):
            block = xbuf[j].reshape(piece * rows, LANES)
            out = jnp.dot(block, table_ref[...], preferred_element_type=jnp.float32)
            tmp[pl.ds(j * piece, piece)] = out.reshape(piece, rows, LANES)
            return carry

        lax.fori_loop(0, 2 * planes, product, 0)

        def butterfly(index, carry):
            r = pl.multiple_of((index // (LANES // 128)) * 16, 16)
            lane = pl.multiple_of((index % (LANES // 128)) * 128, 128)
            values = [tmp[g, pl.ds(r, 16), pl.ds(lane, 128)] for g in range(groups)]
            step = 1
            while step < groups:
                values = [
                    values[g] + values[g + step] if g & step == 0 else values[g - step] - values[g]
                    for g in range(groups)
                ]
                step *= 2
            total = squares[0]
            for g in range(groups):
                rounded = (values[g] * scale).astype(jnp.bfloat16)
                rot[slot, g, pl.ds(r, 16), pl.ds(lane, 128)] = rounded
                exact = rounded.astype(jnp.float32)
                total = total + exact * exact
            squares[0] = total
            return carry

        lax.fori_loop(0, (rows // 16) * (LANES // 128), butterfly, 0)
        for f in range(wide):
            rxr[k, f, pl.ds(0, rows)] = rot[slot, tok * wide + f]
            rxq[k, f, pl.ds(0, rows)] = rot[slot, plane * wide + f]
        send_chunk(k)

    def row_block(k, f):
        left = rxr[k, f].T
        start = pl.multiple_of(f * LANES, LANES)
        for n in range(piece):
            right = jnp.concatenate([rxq[k, core * piece + n], rxm[k, n]], axis=0)
            out = jnp.dot(left, right, preferred_element_type=jnp.float32)
            acc[pl.ds(start, LANES), pl.ds(n * LANES, LANES)] += out

    def joined(k):
        pass_cols(k).wait_recv()
        pass_rows(k, False).wait_recv()

    def gram(k):
        joined(k)

        def body(f, carry):
            row_block(k, f)
            return carry

        lax.fori_loop(0, wide, body, 0)

    def gram_keep(f):
        span = pl.ds(pl.multiple_of(f * LANES, LANES), LANES)
        return pltpu.make_async_copy(acc.at[span], gram_ref.at[span], out_sem.at[f])

    def square_copy(m):
        target = (tok, mate) if m == 4 else (peers[m % 4], col if m < 4 else mate)
        return pltpu.make_async_remote_copy(
            src_ref=squares.at[0], dst_ref=squares.at[m],
            send_sem=s_send.at[m], recv_sem=s_recv.at[m],
            device_id=target, device_id_type=MESH)

    def send_part(k, carry):
        part_copy(k).start()
        return carry

    lax.fori_loop(0, chunks, send_part, 0)
    own_sends(0)
    squares[0] = jnp.zeros((16, 128), jnp.float32)

    def clear(index, carry):
        start = pl.multiple_of(index * 64, 64)
        acc[pl.ds(start, 64)] = jnp.zeros((64, acc.shape[1]), jnp.float32)
        return carry

    lax.fori_loop(0, acc.shape[0] // 64, clear, 0)
    for distance in range(1, planes - 1):
        z_stage(0, distance)
    for k in range(1, LEAD):
        own_sends(k)

    def step(k, carry):
        z_stage(k, planes - 1)
        for copy in loads(k):
            copy.start()

        @pl.when(k + 1 < chunks)
        def _():
            z_stage(k + 1, 1)

        @pl.when(k + LEAD < chunks)
        def _():
            own_sends(k + LEAD)

        @pl.when(k >= RELAY_LAG)
        def _():
            relay(k - RELAY_LAG)

        @pl.when(k >= slots)
        def _():
            sent_chunk(k - slots)

        for copy in loads(k):
            copy.wait()
        rotate(k)

        @pl.when(k + 1 < chunks)
        def _():
            for distance in range(2, planes - 1):
                z_stage(k + 1, distance)

        @pl.when(k >= LAG)
        def _():
            arrivals(k - LAG)

        @pl.when(k > LAG)
        def _():
            gram(k - LAG - 1)

        return carry

    lax.fori_loop(0, chunks, step, 0)
    for m in range(1, 8):
        square_copy(m).start()
    last = chunks - 1
    for k in range(chunks - RELAY_LAG, chunks):
        relay(k)

    def tail(k, carry):
        arrivals(k)
        gram(k - 1)
        return carry

    lax.fori_loop(chunks - LAG, chunks, tail, 0)
    joined(last)

    def final(f, carry):
        row_block(last, f)

        @pl.when(f > 0)
        def _():
            gram_keep(f - 1).start()

        return carry

    lax.fori_loop(0, wide, final, 0)
    gram_keep(wide - 1).start()
    for m in range(1, 8):
        square_copy(m).wait()
    sums = squares[0]
    for m in range(1, 8):
        sums = sums + squares[m]
    square_ref[...] = jnp.full(square_ref.shape, jnp.sum(sums), jnp.float32)

    def drain(k, carry):
        part_copy(k).wait_send()
        for j in range(2 * planes):
            @pl.when(can[0] & (j // 2 <= plane))
            def _():
                z_copy(k, j, 0).wait_send()

            @pl.when(can[1] & (j // 2 >= plane))
            def _():
                z_copy(k, j, 1).wait_send()
        for m in (1, 2):
            @pl.when(relays_here(k, m))
            def _():
                relay_copy(k, m).wait_send()

        for m in (1, 2):
            @pl.when(hops_here(k, m))
            def _():
                hop_forward(k, m).wait_send()

        @pl.when(k >= chunks - slots)
        def _():
            sent_chunk(k)

        pass_rows(k, False).wait_send()
        pass_cols(k).wait_send()
        return carry

    lax.fori_loop(0, chunks, drain, 0)

    def finish(f, carry):
        gram_keep(f).wait()
        return carry

    lax.fori_loop(0, wide, finish, 0)


ROWS = 32
SLOTS = 6
LEAD = 4
RELAY_LAG = 2
LAG = 4


def fits(row_bank, token_ids):
    col_width, tok_rows = row_bank.shape[1], token_ids.shape[0]
    col_count, tok_count = lax.axis_size("col"), lax.axis_size("tok")
    return (
        col_width % LANES == 0
        and tok_count == 4
        and col_count == 8
        and D // tok_count == 2 * col_width
        and tok_rows % (2 * ROWS) == 0
        and tok_rows // (2 * ROWS) >= SLOTS
        and tok_rows * D * 7 // 2 + D // tok_count * col_width * 4 <= 54 * 2**20
    )


def fused(row_bank, token_ids, sign_flips, damping):
    col_width = row_bank.shape[1]
    col_count = lax.axis_size("col")
    tok_count = lax.axis_size("tok")
    tok_rows = token_ids.shape[0]
    planes = col_count // 2
    rows = ROWS
    chunks = tok_rows // 2 // rows
    piece = col_width // LANES
    wide = 2 * piece
    groups = D // LANES
    spread = LANES // BLOCK
    inner = jnp.asarray(np.kron(np.eye(spread), sylvester(BLOCK)), jnp.bfloat16)
    outer = jnp.asarray(np.kron(sylvester(spread), np.eye(BLOCK)), jnp.bfloat16)
    signs = sign_flips.astype(jnp.bfloat16)[:, None]
    picked = row_bank.at[token_ids].get(mode="promise_in_bounds")
    parts = []
    for g in range(piece):
        part = picked[:, g * LANES : (g + 1) * LANES]
        table = inner * signs[g * LANES : (g + 1) * LANES]
        part = jnp.dot(part, table, preferred_element_type=jnp.float32).astype(jnp.bfloat16)
        parts.append(part.reshape(2, chunks, rows, LANES))
    half = jnp.stack(parts, axis=2)
    any_space = pl.BlockSpec(memory_space=pl.ANY)
    vmem = pl.BlockSpec(memory_space=pltpu.VMEM)
    dma = pltpu.SemaphoreType.DMA
    height = D // tok_count
    gram, squares, _, _ = pl.pallas_call(
        functools.partial(fused_kernel, planes, chunks, rows, piece, SLOTS, 1.0 / math.sqrt(D)),
        out_shape=(
            jax.ShapeDtypeStruct((height, col_width), jnp.float32),
            jax.ShapeDtypeStruct((8, 128), jnp.float32),
            jax.ShapeDtypeStruct((chunks, col_count, piece, rows, LANES), jnp.bfloat16),
            jax.ShapeDtypeStruct((2, chunks, wide, rows, LANES), jnp.bfloat16),
        ),
        in_specs=[any_space, vmem],
        out_specs=(any_space, vmem, any_space, any_space),
        scratch_shapes=[
            pltpu.VMEM((col_count, piece, rows, LANES), jnp.bfloat16),
            pltpu.VMEM((groups, rows, LANES), jnp.float32),
            pltpu.VMEM((SLOTS, groups, rows, LANES), jnp.bfloat16),
            pltpu.VMEM((chunks, wide, 8 * rows, LANES), jnp.bfloat16),
            pltpu.VMEM((chunks, wide, 4 * rows, LANES), jnp.bfloat16),
            pltpu.VMEM((chunks, piece, 4 * rows, LANES), jnp.bfloat16),
            pltpu.VMEM((height, col_width), jnp.float32),
            pltpu.VMEM((8, 16, 128), jnp.float32),
            dma((chunks,)), dma((chunks,)),
            dma((chunks, col_count, 2)), dma((chunks, col_count)),
            dma((chunks, 4)), dma((chunks, 4)),
            dma((chunks, 5)), dma((chunks, 4)),
            dma((chunks, 3)), dma((chunks, 3)),
            dma((chunks, 2)), dma((chunks, 2)),
            dma((8,)), dma((8,)),
            dma((planes + 1,)), dma((wide,)),
        ],
        compiler_params=pltpu.CompilerParams(
            collective_id=0, has_side_effects=True, vmem_limit_bytes=67043328
        ),
    )(half, outer)
    tokens_all = tok_rows * tok_count
    mean_diag = squares[0, 0] / tokens_all / D
    return damped(gram / tokens_all, damping, mean_diag)


def damped(gram_block, damping, mean_diag):
    block_rows, col_width = gram_block.shape
    row_index = lax.axis_index("tok") * block_rows + lax.broadcasted_iota(
        jnp.int32, gram_block.shape, 0
    )
    col_index = lax.axis_index("col") * col_width + lax.broadcasted_iota(
        jnp.int32, gram_block.shape, 1
    )
    on_diag = (row_index == col_index).astype(jnp.float32)
    return gram_block + damping[0] * mean_diag * on_diag


def plain(row_bank, token_ids, sign_flips, damping):
    col_width = row_bank.shape[1]
    col_count = lax.axis_size("col")
    tok_count = lax.axis_size("tok")
    tok_rows = token_ids.shape[0]
    groups = D // BLOCK
    scale = 1.0 / math.sqrt(D)
    inner_table = hadamard(BLOCK)
    outer_table = hadamard(groups)
    col_start = lax.axis_index("col") * col_width
    picked = jnp.take(row_bank, token_ids, axis=0) * sign_flips.astype(jnp.bfloat16)[None, :]
    shaped = picked.reshape(picked.shape[0], -1, BLOCK)
    turned = jnp.einsum("rab,bc->rac", shaped, inner_table, preferred_element_type=jnp.float32)
    half_turned = turned.astype(jnp.bfloat16).reshape(picked.shape)
    grouped = half_turned.reshape(col_count, tok_rows // col_count, col_width)
    block = lax.all_to_all(grouped, "col", split_axis=0, concat_axis=2, tiled=True)[0]
    shaped = block.reshape(block.shape[0], groups, BLOCK)
    turned = (
        jnp.einsum("rab,ac->rcb", shaped, outer_table, preferred_element_type=jnp.float32) * scale
    )
    finished = turned.astype(jnp.bfloat16).reshape(block.shape)[None]
    squares = jnp.sum(jnp.square(finished.astype(jnp.float32)))
    tokens_all = tok_rows * tok_count
    square_sum = lax.psum(squares, ("tok", "col"))
    mean_diag = square_sum / tokens_all / D
    flat = lax.all_gather(finished, "col", axis=1, tiled=True).reshape(-1, D)
    own_cols = lax.dynamic_slice_in_dim(flat, col_start, col_width, 1)
    partial_sum = lax.dot_general(
        flat, own_cols, (((0,), (0,)), ((), ())), preferred_element_type=jnp.float32
    )
    gram_block = lax.psum_scatter(partial_sum, "tok", scatter_dimension=0, tiled=True) / tokens_all
    return damped(gram_block, damping, mean_diag)


def shards(row_bank, token_ids, sign_flips, damping):
    run = fused if fits(row_bank, token_ids) else plain
    return run(row_bank, token_ids, sign_flips, damping)


def solution(mesh):
    in_specs = (P(None, "col"), P("tok"), P("col"), P())
    out_specs = P("tok", "col")
    return jax.shard_map(shards, mesh=mesh, in_specs=in_specs, out_specs=out_specs, check_vma=False)
```

```python
import functools
import math

import jax
import jax.numpy as jnp
import numpy as np
from jax import lax
from jax.experimental import pallas as pl
from jax.experimental.pallas import tpu as pltpu
from jax.sharding import PartitionSpec as P

D = 8192
BLOCK = 32
LANES = 512
MESH = pl.DeviceIdType.MESH


def hadamard(order):
    index_range = jnp.arange(order, dtype=jnp.int32)
    anded = jnp.bitwise_and(index_range[:, None], index_range[None, :])
    parity = jnp.zeros((order, order), jnp.int32)
    for bit_place in range(int(order).bit_length()):
        parity = parity + jnp.bitwise_and(jnp.right_shift(anded, bit_place), 1)
    return (1 - 2 * jnp.bitwise_and(parity, 1)).astype(jnp.bfloat16)


def sylvester(order):
    table = np.ones((1, 1))
    while table.shape[0] < order:
        table = np.block([[table, table], [table, -table]])
    return table


def fused_kernel(
    planes, chunks, rows, piece, slots, scale, tokens_all,
    picked_ref, sign_ref, damp_ref, inner_ref, table_ref,
    gram_ref, full_ref, hop_ref,
    pick, half, xbuf, tmp, rot, rxr, rxq, rxm, acc, squares,
    part_send, part_recv, z_send, z_recv, sent, col_recv, in_recv, relay_send,
    h_send, h_recv, m_send, m_recv, s_send, s_recv, pick_sem, load_sem, out_sem,
):
    tok = lax.axis_index("tok")
    col = lax.axis_index("col")
    plane, core = col // 2, col % 2
    mate = plane * 2 + (1 - core)
    ypos, xpos = tok // 2, tok % 2
    peers = {1: ypos * 2 + (1 - xpos), 2: (1 - ypos) * 2 + xpos, 3: 3 - tok}
    wide = 2 * piece
    role = ((ypos + plane // 2) % 2) * 2 + (xpos + plane) % 2

    barrier = pltpu.get_barrier_semaphore()
    greet = [(tok, mate)]
    for m in (1, 2, 3):
        greet.append((peers[m], col))
        greet.append((peers[m], mate))
    for m in range(1, planes):
        greet.append((tok, ((plane + m) % planes) * 2 + core))
    for device in greet:
        pl.semaphore_signal(barrier, inc=1, device_id=device, device_id_type=MESH)

    def pick_copies(k):
        slot = k % 2
        return [
            pltpu.make_async_copy(
                picked_ref.at[side, k], pick.at[slot, side], pick_sem.at[slot, side])
            for side in (0, 1)
        ]

    def fetch(k):
        for copy in pick_copies(k):
            copy.start()

    def turn_half(k):
        slot = k % 2
        for copy in pick_copies(k):
            copy.wait()
        signed = []
        for g in range(piece):
            lanes = pl.ds(g * LANES, LANES)
            signs = sign_ref[:, lanes].astype(jnp.float32).astype(jnp.bfloat16)
            for side in (0, 1):
                signed.append(pick[slot, side, :, lanes] * signs)
        out = jnp.dot(
            jnp.concatenate(signed, axis=0), inner_ref[...], preferred_element_type=jnp.float32
        ).astype(jnp.bfloat16)
        for g in range(piece):
            for side in (0, 1):
                start = (2 * g + side) * rows
                half[side, k, g] = out[start : start + rows]

    def part_copy(k):
        return pltpu.make_async_remote_copy(
            src_ref=half.at[1 - core, k], dst_ref=full_ref.at[k, col],
            send_sem=part_send.at[k % RING], recv_sem=part_recv.at[k],
            device_id=(tok, mate), device_id_type=MESH)

    def part_arrival(k):
        return pltpu.make_async_remote_copy(
            src_ref=half.at[1 - core, k], dst_ref=full_ref.at[k, mate],
            send_sem=part_send.at[k % RING], recv_sem=part_recv.at[k],
            device_id=(tok, mate), device_id_type=MESH)

    def z_copy(k, origin, way, source, target):
        own = (origin == plane) & (way == 1)
        return pltpu.make_async_remote_copy(
            src_ref=source, dst_ref=target,
            send_sem=z_send.at[k % RING, jnp.where(own, planes, origin)],
            recv_sem=z_recv.at[k, origin],
            device_id=(tok, col + 2 - 4 * way), device_id_type=MESH)

    def z_both(k, origin, way):
        both = full_ref.at[k, pl.ds(2 * origin, 2)]
        return z_copy(k, origin, way, both, both)

    can = {0: plane < planes - 1, 1: plane > 0}

    def own_sends(k):
        for way in (0, 1):
            @pl.when(can[way])
            def _():
                z_copy(k, plane, way, half.at[core, k], full_ref.at[k, col]).start()
        part_arrival(k).wait_recv()
        for way in (0, 1):
            @pl.when(can[way])
            def _():
                z_copy(k, plane, way, full_ref.at[k, mate], full_ref.at[k, mate]).start()

    def z_stage(k, distance):
        for way, origin in ((0, plane - distance), (1, plane + distance)):
            @pl.when((origin >= 0) & (origin < planes))
            def _():
                z_both(k, origin, way).wait_recv()

                @pl.when(can[way])
                def _():
                    z_both(k, origin, way).start()

    def place(k, m):
        return pl.ds(pl.multiple_of((k % 2) * 4 * rows + m * rows, rows), rows)

    def col_copy(k, m):
        return pltpu.make_async_remote_copy(
            src_ref=rot.at[k % slots, pl.ds(plane * wide, wide)],
            dst_ref=rxq.at[k // 2, :, place(k, m)],
            send_sem=sent.at[k % slots], recv_sem=col_recv.at[k],
            device_id=(peers[m], col), device_id_type=MESH)

    def relay_copy(k, m):
        return pltpu.make_async_remote_copy(
            src_ref=rxq.at[k // 2, :, place(k, m)],
            dst_ref=rxq.at[k // 2, :, place(k, 3)],
            send_sem=relay_send.at[k % RING, m - 1], recv_sem=in_recv.at[k // 2],
            device_id=(peers[3 - m], col), device_id_type=MESH)

    def row_copy(k, m):
        return pltpu.make_async_remote_copy(
            src_ref=rot.at[k % slots, pl.ds(peers[m] * wide, wide)],
            dst_ref=rxr.at[k // 2, :, place(k, m)],
            send_sem=sent.at[k % slots], recv_sem=in_recv.at[k // 2],
            device_id=(peers[m], col), device_id_type=MESH)

    def hop_copy(k, m):
        return pltpu.make_async_remote_copy(
            src_ref=rot.at[k % slots, pl.ds(peers[3] * wide, wide)],
            dst_ref=hop_ref.at[m - 1, k],
            send_sem=sent.at[k % slots], recv_sem=h_recv.at[k, m - 1],
            device_id=(peers[m], col), device_id_type=MESH)

    def hop_forward(k, m):
        return pltpu.make_async_remote_copy(
            src_ref=hop_ref.at[m - 1, k],
            dst_ref=rxr.at[k // 2, :, place(k, 3)],
            send_sem=h_send.at[k % RING, m - 1], recv_sem=in_recv.at[k // 2],
            device_id=(peers[3 - m], col), device_id_type=MESH)

    def turn(k):
        return (k + 2 * core) % 4

    def y_first(k, sender):
        phase = turn(k)
        return (
            ((sender == 0) & (phase % 2 == 0))
            | ((sender == 2) & (phase < 3))
            | ((sender == 1) & (phase == 0))
        )

    def hops_here(k, m):
        if m == 2:
            return y_first(k, (role + 2) % 4)
        sender = role + 1 - 2 * (role % 2)
        return (sender != 3) & jnp.logical_not(y_first(k, sender))

    def relays_here(k, m):
        even = turn(k) % 2 == 0
        if m == 1:
            return (role >= 2) | ((role == 1) & even)
        return (role == 3) | ((role == 2) & (turn(k) % 2 == 1))

    def send_chunk(k):
        for m in (1, 2):
            col_copy(k, m).start()
        hop = y_first(k, role)

        @pl.when(hop)
        def _():
            hop_copy(k, 2).start()

        @pl.when(jnp.logical_not(hop) & (role != 3))
        def _():
            hop_copy(k, 1).start()

        for m in (1, 2):
            @pl.when(role != m)
            def _():
                row_copy(k, m).start()

    def blocks(count, send_sem, recv_sem):
        area = hop_ref.at[0, pl.ds(0, count)]
        return pltpu.make_async_remote_copy(
            src_ref=area, dst_ref=area, send_sem=send_sem, recv_sem=recv_sem,
            device_id=(peers[1], col), device_id_type=MESH)

    def sent_chunk(k):
        slot = sent.at[k % slots]

        @pl.when(role == 0)
        def _():
            blocks(5, slot, col_recv.at[0]).wait_send()

        @pl.when(role != 0)
        def _():
            blocks(4, slot, col_recv.at[0]).wait_send()

    def relay(k):
        blocks(2, sent.at[0], col_recv.at[k]).wait_recv()
        for m in (1, 2):
            @pl.when(relays_here(k, m))
            def _():
                relay_copy(k, m).start()

        for m in (1, 2):
            @pl.when(hops_here(k, m))
            def _():
                hop_copy(k, m).wait_recv()
                hop_forward(k, m).start()

    def pass_rows(p, same):
        source = rxq.at[p] if same else rxr.at[p, :, pl.ds(0, 8 * rows)]
        return pltpu.make_async_remote_copy(
            src_ref=source, dst_ref=rxr.at[p, :, pl.ds(8 * rows, 8 * rows)],
            send_sem=m_send.at[p, 0], recv_sem=m_recv.at[p, 0],
            device_id=(tok, mate), device_id_type=MESH)

    def pass_cols(p):
        return pltpu.make_async_remote_copy(
            src_ref=rxq.at[p, pl.ds((1 - core) * piece, piece)], dst_ref=rxm.at[p],
            send_sem=m_send.at[p, 1], recv_sem=m_recv.at[p, 1],
            device_id=(tok, mate), device_id_type=MESH)

    def arrivals(p):
        @pl.when(role != 0)
        def _():
            blocks(8, sent.at[0], in_recv.at[p]).wait_recv()
            pass_rows(p, False).start()

        @pl.when(role == 0)
        def _():
            blocks(2, sent.at[0], in_recv.at[p]).wait_recv()
            pass_rows(p, True).start()
            for f in range(wide):
                rxr[p, f, pl.ds(0, 8 * rows)] = rxq[p, f]

        pass_cols(p).start()

    def loads(k):
        copies = [pltpu.make_async_copy(full_ref.at[k, mate], xbuf.at[mate], load_sem.at[1])]
        for m in range(1, planes):
            other = ((plane + m) % planes) * 2
            copies.append(pltpu.make_async_copy(
                full_ref.at[k, pl.ds(other, 2)], xbuf.at[pl.ds(other, 2)], load_sem.at[1 + m]))
        return copies

    groups = 2 * planes * piece

    def rotate(k):
        slot = k % slots

        block = xbuf[...].reshape(groups * rows, LANES)
        out = jnp.dot(block, table_ref[...], preferred_element_type=jnp.float32)
        tmp[...] = out.reshape(groups, rows, LANES)

        def butterfly(index, carry):
            r = pl.multiple_of((index // (LANES // 128)) * 16, 16)
            lane = pl.multiple_of((index % (LANES // 128)) * 128, 128)
            values = [tmp[g, pl.ds(r, 16), pl.ds(lane, 128)] for g in range(groups)]
            step = 1
            while step < groups:
                values = [
                    values[g] + values[g + step] if g & step == 0 else values[g - step] - values[g]
                    for g in range(groups)
                ]
                step *= 2
            total = squares[0]
            for g in range(groups):
                rounded = (values[g] * scale).astype(jnp.bfloat16)
                rot[slot, g, pl.ds(r, 16), pl.ds(lane, 128)] = rounded
                exact = rounded.astype(jnp.float32)
                total = total + exact * exact
            squares[0] = total
            return carry

        lax.fori_loop(0, (rows // 16) * (LANES // 128), butterfly, 0)
        for f in range(wide):
            rxr[k // 2, f, place(k, 0)] = rot[slot, tok * wide + f]
            rxq[k // 2, f, place(k, 0)] = rot[slot, plane * wide + f]
        send_chunk(k)

    def row_block(k, f):
        left = rxr[k, f].T
        start = pl.multiple_of(f * LANES, LANES)
        for n in range(piece):
            right = jnp.concatenate([rxq[k, core * piece + n], rxm[k, n]], axis=0)
            out = jnp.dot(left, right, preferred_element_type=jnp.float32)
            acc[pl.ds(start, LANES), pl.ds(n * LANES, LANES)] += out

    def joined(k):
        pass_cols(k).wait_recv()
        pass_rows(k, False).wait_recv()

    def gram(k):
        joined(k)

        def body(f, carry):
            row_block(k, f)
            return carry

        lax.fori_loop(0, wide, body, 0)

    def gram_keep(f):
        span = pl.ds(pl.multiple_of(f * LANES, LANES), LANES)
        return pltpu.make_async_copy(acc.at[span], gram_ref.at[span], out_sem.at[f])

    def square_copy(m):
        target = (tok, mate) if m == 4 else (peers[m % 4], col if m < 4 else mate)
        return pltpu.make_async_remote_copy(
            src_ref=squares.at[0], dst_ref=squares.at[m],
            send_sem=s_send.at[0], recv_sem=s_recv.at[0],
            device_id=target, device_id_type=MESH)

    def squares_done():
        return pltpu.make_async_remote_copy(
            src_ref=squares.at[pl.ds(1, 7)], dst_ref=squares.at[pl.ds(1, 7)],
            send_sem=s_send.at[0], recv_sem=s_recv.at[0],
            device_id=(tok, mate), device_id_type=MESH)

    fetch(0)
    fetch(1)
    turn_half(0)
    pl.semaphore_wait(barrier, len(greet))
    part_copy(0).start()
    own_sends(0)
    fetch(2)
    squares[0] = jnp.zeros((16, 128), jnp.float32)

    def clear(index, carry):
        start = pl.multiple_of(index * 64, 64)
        acc[pl.ds(start, 64)] = jnp.zeros((64, acc.shape[1]), jnp.float32)
        return carry

    lax.fori_loop(0, acc.shape[0] // 64, clear, 0)
    for distance in range(1, planes - 1):
        turn_half(distance)
        fetch(distance + 2)
        part_copy(distance).start()
        z_stage(0, distance)
        own_sends(distance)
    for k in range(planes - 1, LEAD + 1):
        turn_half(k)
        fetch(k + 2)
        part_copy(k).start()
    for k in range(planes - 1, LEAD):
        own_sends(k)

    def drain(k):
        part_copy(k).wait_send()
        for origin in range(planes):
            @pl.when(can[0] & (origin <= plane))
            def _():
                z_both(k, origin, 0).wait_send()

            @pl.when(can[1] & (origin >= plane))
            def _():
                z_both(k, origin, 1).wait_send()
        for m in (1, 2):
            @pl.when(relays_here(k, m))
            def _():
                relay_copy(k, m).wait_send()

            @pl.when(hops_here(k, m))
            def _():
                hop_forward(k, m).wait_send()

    def step(k, carry):
        z_stage(k, planes - 1)
        for copy in loads(k):
            copy.start()

        @pl.when(k + 1 < chunks)
        def _():
            z_stage(k + 1, 1)

        @pl.when(k + LEAD < chunks)
        def _():
            own_sends(k + LEAD)

        @pl.when(k + LEAD + 1 < chunks)
        def _():
            turn_half(k + LEAD + 1)
            part_copy(k + LEAD + 1).start()

        @pl.when(k + LEAD + 3 < chunks)
        def _():
            fetch(k + LEAD + 3)

        @pl.when(k >= RELAY_LAG)
        def _():
            relay(k - RELAY_LAG)

        @pl.when(k >= slots)
        def _():
            sent_chunk(k - slots)

        for copy in loads(k):
            copy.wait()
        xbuf[col] = half[core, k]
        rotate(k)

        @pl.when(k + 1 < chunks)
        def _():
            for distance in range(2, planes - 1):
                z_stage(k + 1, distance)

        @pl.when((k % 2 == 1) & (k // 2 >= LAG))
        def _():
            arrivals(k // 2 - LAG)

        @pl.when((k % 2 == 1) & (k // 2 > LAG))
        def _():
            gram(k // 2 - LAG - 1)

        @pl.when(k >= DRAIN)
        def _():
            drain(k - DRAIN)

        return carry

    lax.fori_loop(0, chunks, step, 0)
    for m in range(1, 8):
        square_copy(m).start()
    pairs = chunks // 2
    last = pairs - 1
    for k in range(chunks - RELAY_LAG, chunks):
        relay(k)

    def tail(p, carry):
        arrivals(p)
        gram(p - 1)
        for k in (0, 1):
            drain(2 * (p + LAG) - DRAIN + k)
        return carry

    lax.fori_loop(pairs - LAG, pairs, tail, 0)
    squares_done().wait()
    sums = squares[0]
    for m in range(1, 8):
        sums = sums + squares[m]
    lift = damp_ref[0] * (jnp.sum(sums) / D)
    joined(last)

    def final(f, carry):
        left = rxr[last, f].T
        start = pl.multiple_of(f * LANES, LANES)
        for n in range(piece):
            right = jnp.concatenate([rxq[last, core * piece + n], rxm[last, n]], axis=0)
            out = jnp.dot(left, right, preferred_element_type=jnp.float32)
            here = (pl.ds(start, LANES), pl.ds(n * LANES, LANES))
            acc[here] += out

            @pl.when((role == 0) & (f == core * piece + n))
            def _():
                row = lax.broadcasted_iota(jnp.int32, (LANES, LANES), 0)
                column = lax.broadcasted_iota(jnp.int32, (LANES, LANES), 1)
                acc[here] += lift * (row == column).astype(jnp.float32)

        @pl.when(f > 0)
        def _():
            gram_keep(f - 1).start()

        return carry

    lax.fori_loop(0, wide, final, 0)
    gram_keep(wide - 1).start()

    def rest(k, carry):
        @pl.when(k < pairs)
        def _():
            pass_rows(k, False).wait_send()
            pass_cols(k).wait_send()

        @pl.when(k >= chunks - DRAIN + 2 * LAG)
        def _():
            drain(k)

        @pl.when(k >= chunks - slots)
        def _():
            sent_chunk(k)

        return carry

    lax.fori_loop(0, chunks, rest, 0)

    def finish(f, carry):
        gram_keep(f).wait()
        return carry

    lax.fori_loop(0, wide, finish, 0)


ROWS = 16
SLOTS = 12
LEAD = 6
RELAY_LAG = 3
LAG = 3
DRAIN = 12
RING = 20


def fits(row_bank, token_ids):
    col_width, tok_rows = row_bank.shape[1], token_ids.shape[0]
    col_count, tok_count = lax.axis_size("col"), lax.axis_size("tok")
    return (
        col_width % LANES == 0
        and tok_count == 4
        and col_count == 8
        and D // tok_count == 2 * col_width
        and tok_rows % (4 * ROWS) == 0
        and tok_rows // (2 * ROWS) >= DRAIN
        and tok_rows * D * 7 // 2 + D // tok_count * col_width * 4 <= 54 * 2**20
    )


def fused(row_bank, token_ids, sign_flips, damping):
    col_width = row_bank.shape[1]
    col_count = lax.axis_size("col")
    tok_count = lax.axis_size("tok")
    tok_rows = token_ids.shape[0]
    planes = col_count // 2
    rows = ROWS
    chunks = tok_rows // 2 // rows
    piece = col_width // LANES
    wide = 2 * piece
    groups = D // LANES
    spread = LANES // BLOCK
    inner = jnp.asarray(np.kron(np.eye(spread), sylvester(BLOCK)), jnp.bfloat16)
    outer = jnp.asarray(np.kron(sylvester(spread), np.eye(BLOCK)), jnp.bfloat16)
    picked = row_bank.at[token_ids].get(
        mode="promise_in_bounds", wrap_negative_indices=False
    ).reshape(2, chunks, rows, col_width)
    any_space = pl.BlockSpec(memory_space=pl.ANY)
    vmem = pl.BlockSpec(memory_space=pltpu.VMEM)
    dma = pltpu.SemaphoreType.DMA
    height = D // tok_count
    gram, _, _ = pl.pallas_call(
        functools.partial(fused_kernel, planes, chunks, rows, piece, SLOTS, 1.0 / math.sqrt(D),
                          tok_rows * tok_count),
        out_shape=(
            jax.ShapeDtypeStruct((height, col_width), jnp.float32),
            jax.ShapeDtypeStruct((chunks, col_count, piece, rows, LANES), jnp.bfloat16),
            jax.ShapeDtypeStruct((2, chunks, wide, rows, LANES), jnp.bfloat16),
        ),
        in_specs=[any_space, vmem, pl.BlockSpec(memory_space=pltpu.SMEM), vmem, vmem],
        out_specs=(any_space, any_space, any_space),
        scratch_shapes=[
            pltpu.VMEM((2, 2, rows, col_width), jnp.bfloat16),
            pltpu.VMEM((2, chunks, piece, rows, LANES), jnp.bfloat16),
            pltpu.VMEM((col_count, piece, rows, LANES), jnp.bfloat16),
            pltpu.VMEM((groups, rows, LANES), jnp.float32),
            pltpu.VMEM((SLOTS, groups, rows, LANES), jnp.bfloat16),
            pltpu.VMEM((chunks // 2, wide, 16 * rows, LANES), jnp.bfloat16),
            pltpu.VMEM((chunks // 2, wide, 8 * rows, LANES), jnp.bfloat16),
            pltpu.VMEM((chunks // 2, piece, 8 * rows, LANES), jnp.bfloat16),
            pltpu.VMEM((height, col_width), jnp.float32),
            pltpu.VMEM((8, 16, 128), jnp.float32),
            dma((RING,)), dma((chunks,)),
            dma((RING, planes + 1)), dma((chunks, planes)),
            dma((SLOTS,)), dma((chunks,)), dma((chunks // 2,)), dma((RING, 2)),
            dma((RING, 2)), dma((chunks, 2)),
            dma((chunks // 2, 2)), dma((chunks // 2, 2)),
            dma((1,)), dma((1,)),
            dma((2, 2)), dma((planes + 1,)), dma((wide,)),
        ],
        compiler_params=pltpu.CompilerParams(
            collective_id=0, has_side_effects=True, vmem_limit_bytes=67043328
        ),
    )(picked, sign_flips[None, :], damping, inner, outer)
    return gram * jnp.float32(1.0 / (tok_rows * tok_count))


def damped(gram_block, damping, mean_diag):
    block_rows, col_width = gram_block.shape
    row_index = lax.axis_index("tok") * block_rows + lax.broadcasted_iota(
        jnp.int32, gram_block.shape, 0
    )
    col_index = lax.axis_index("col") * col_width + lax.broadcasted_iota(
        jnp.int32, gram_block.shape, 1
    )
    on_diag = (row_index == col_index).astype(jnp.float32)
    return gram_block + damping[0] * mean_diag * on_diag


def plain(row_bank, token_ids, sign_flips, damping):
    col_width = row_bank.shape[1]
    col_count = lax.axis_size("col")
    tok_count = lax.axis_size("tok")
    tok_rows = token_ids.shape[0]
    groups = D // BLOCK
    scale = 1.0 / math.sqrt(D)
    inner_table = hadamard(BLOCK)
    outer_table = hadamard(groups)
    col_start = lax.axis_index("col") * col_width
    picked = jnp.take(row_bank, token_ids, axis=0) * sign_flips.astype(jnp.bfloat16)[None, :]
    shaped = picked.reshape(picked.shape[0], -1, BLOCK)
    turned = jnp.einsum("rab,bc->rac", shaped, inner_table, preferred_element_type=jnp.float32)
    half_turned = turned.astype(jnp.bfloat16).reshape(picked.shape)
    grouped = half_turned.reshape(col_count, tok_rows // col_count, col_width)
    block = lax.all_to_all(grouped, "col", split_axis=0, concat_axis=2, tiled=True)[0]
    shaped = block.reshape(block.shape[0], groups, BLOCK)
    turned = (
        jnp.einsum("rab,ac->rcb", shaped, outer_table, preferred_element_type=jnp.float32) * scale
    )
    finished = turned.astype(jnp.bfloat16).reshape(block.shape)[None]
    squares = jnp.sum(jnp.square(finished.astype(jnp.float32)))
    tokens_all = tok_rows * tok_count
    square_sum = lax.psum(squares, ("tok", "col"))
    mean_diag = square_sum / tokens_all / D
    flat = lax.all_gather(finished, "col", axis=1, tiled=True).reshape(-1, D)
    own_cols = lax.dynamic_slice_in_dim(flat, col_start, col_width, 1)
    partial_sum = lax.dot_general(
        flat, own_cols, (((0,), (0,)), ((), ())), preferred_element_type=jnp.float32
    )
    gram_block = lax.psum_scatter(partial_sum, "tok", scatter_dimension=0, tiled=True) / tokens_all
    return damped(gram_block, damping, mean_diag)


def shards(row_bank, token_ids, sign_flips, damping):
    run = fused if fits(row_bank, token_ids) else plain
    return run(row_bank, token_ids, sign_flips, damping)


def solution(mesh):
    in_specs = (P(None, "col"), P("tok"), P("col"), P())
    out_specs = P("tok", "col")
    return jax.shard_map(shards, mesh=mesh, in_specs=in_specs, out_specs=out_specs, check_vma=False)
```

```python
import functools
import math

import jax
import jax.numpy as jnp
import numpy as np
from jax import lax
from jax.experimental import pallas as pl
from jax.experimental.pallas import tpu as pltpu
from jax.sharding import PartitionSpec as P

D = 8192
BLOCK = 32
LANES = 512
MESH = pl.DeviceIdType.MESH


def hadamard(order):
    index_range = jnp.arange(order, dtype=jnp.int32)
    anded = jnp.bitwise_and(index_range[:, None], index_range[None, :])
    parity = jnp.zeros((order, order), jnp.int32)
    for bit_place in range(int(order).bit_length()):
        parity = parity + jnp.bitwise_and(jnp.right_shift(anded, bit_place), 1)
    return (1 - 2 * jnp.bitwise_and(parity, 1)).astype(jnp.bfloat16)


def sylvester(order):
    table = np.ones((1, 1))
    while table.shape[0] < order:
        table = np.block([[table, table], [table, -table]])
    return table


def fused_kernel(
    planes, chunks, rows, piece, slots, scale, tokens_all,
    picked_ref, sign_ref, damp_ref, inner_ref, table_ref,
    gram_ref, full_ref, hop_ref,
    pick, half, xbuf, tmp, rot, rxr, rxq, rxm, acc, squares,
    part_send, part_recv, z_send, z_recv, sent, col_recv, in_recv, relay_send,
    h_send, h_recv, m_send, m_recv, s_send, s_recv, pick_sem, load_sem, out_sem,
):
    tok = lax.axis_index("tok")
    col = lax.axis_index("col")
    plane, core = col // 2, col % 2
    mate = plane * 2 + (1 - core)
    ypos, xpos = tok // 2, tok % 2
    peers = {1: ypos * 2 + (1 - xpos), 2: (1 - ypos) * 2 + xpos, 3: 3 - tok}
    wide = 2 * piece
    role = ((ypos + plane // 2) % 2) * 2 + (xpos + plane) % 2

    barrier = pltpu.get_barrier_semaphore()
    greet = [(tok, mate)]
    for m in (1, 2, 3):
        greet.append((peers[m], col))
        greet.append((peers[m], mate))
    for m in range(1, planes):
        greet.append((tok, ((plane + m) % planes) * 2 + core))
    for device in greet:
        pl.semaphore_signal(barrier, inc=1, device_id=device, device_id_type=MESH)

    def pick_copies(k):
        slot = k % 2
        return [
            pltpu.make_async_copy(
                picked_ref.at[side, k], pick.at[slot, side], pick_sem.at[slot, side])
            for side in (0, 1)
        ]

    def fetch(k):
        for copy in pick_copies(k):
            copy.start()

    def turn_half(k):
        slot = k % 2
        for copy in pick_copies(k):
            copy.wait()
        signed = []
        for g in range(piece):
            lanes = pl.ds(g * LANES, LANES)
            signs = sign_ref[:, lanes].astype(jnp.float32).astype(jnp.bfloat16)
            for side in (0, 1):
                signed.append(pick[slot, side, :, lanes] * signs)
        out = jnp.dot(
            jnp.concatenate(signed, axis=0), inner_ref[...], preferred_element_type=jnp.float32
        ).astype(jnp.bfloat16)
        for g in range(piece):
            for side in (0, 1):
                start = (2 * g + side) * rows
                half[side, k, g] = out[start : start + rows]

    def part_copy(k):
        return pltpu.make_async_remote_copy(
            src_ref=half.at[1 - core, k], dst_ref=full_ref.at[k, col],
            send_sem=part_send.at[k % RING], recv_sem=part_recv.at[k],
            device_id=(tok, mate), device_id_type=MESH)

    def part_arrival(k):
        return pltpu.make_async_remote_copy(
            src_ref=half.at[1 - core, k], dst_ref=full_ref.at[k, mate],
            send_sem=part_send.at[k % RING], recv_sem=part_recv.at[k],
            device_id=(tok, mate), device_id_type=MESH)

    def z_copy(k, origin, way, source, target):
        return pltpu.make_async_remote_copy(
            src_ref=source, dst_ref=target,
            send_sem=z_send.at[k % RING, origin + way],
            recv_sem=z_recv.at[k, origin - way],
            device_id=(tok, col + 2 - 4 * way), device_id_type=MESH)

    def z_both(k, origin, way):
        both = full_ref.at[k, pl.ds(2 * origin, 2)]
        return z_copy(k, origin, way, both, both)

    can = {0: plane < planes - 1, 1: plane > 0}

    def own_sends(k):
        for way in (0, 1):
            @pl.when(can[way])
            def _():
                z_copy(k, plane, way, half.at[core, k], full_ref.at[k, col]).start()
        part_arrival(k).wait_recv()
        for way in (0, 1):
            @pl.when(can[way])
            def _():
                z_copy(k, plane, way, full_ref.at[k, mate], full_ref.at[k, mate]).start()

    def z_stage(k, distance):
        for way, origin in ((0, plane - distance), (1, plane + distance)):
            @pl.when((origin >= 0) & (origin < planes))
            def _():
                z_both(k, origin, way).wait_recv()

                @pl.when(can[way])
                def _():
                    z_both(k, origin, way).start()

    def place(k, m):
        return pl.ds(pl.multiple_of((k % 2) * 4 * rows + m * rows, rows), rows)

    def col_copy(k, m):
        return pltpu.make_async_remote_copy(
            src_ref=rot.at[k % slots, pl.ds(plane * wide, wide)],
            dst_ref=rxq.at[k // 2, :, place(k, m)],
            send_sem=sent.at[k % slots], recv_sem=col_recv.at[k],
            device_id=(peers[m], col), device_id_type=MESH)

    def relay_copy(k, m):
        return pltpu.make_async_remote_copy(
            src_ref=rxq.at[k // 2, :, place(k, m)],
            dst_ref=rxq.at[k // 2, :, place(k, 3)],
            send_sem=relay_send.at[k % RING, m - 1], recv_sem=in_recv.at[k // 2],
            device_id=(peers[3 - m], col), device_id_type=MESH)

    def row_copy(k, m):
        return pltpu.make_async_remote_copy(
            src_ref=rot.at[k % slots, pl.ds(peers[m] * wide, wide)],
            dst_ref=rxr.at[k // 2, :, place(k, m)],
            send_sem=sent.at[k % slots], recv_sem=in_recv.at[k // 2],
            device_id=(peers[m], col), device_id_type=MESH)

    def hop_copy(k, m):
        return pltpu.make_async_remote_copy(
            src_ref=rot.at[k % slots, pl.ds(peers[3] * wide, wide)],
            dst_ref=hop_ref.at[m - 1, k],
            send_sem=sent.at[k % slots], recv_sem=h_recv.at[k],
            device_id=(peers[m], col), device_id_type=MESH)

    def hop_forward(k, m):
        return pltpu.make_async_remote_copy(
            src_ref=hop_ref.at[m - 1, k],
            dst_ref=rxr.at[k // 2, :, place(k, 3)],
            send_sem=h_send.at[k % RING, m - 1], recv_sem=in_recv.at[k // 2],
            device_id=(peers[3 - m], col), device_id_type=MESH)

    def turn(k):
        return (k + 2 * core) % 4

    def y_first(k, sender):
        phase = turn(k)
        return (
            ((sender == 0) & (phase % 2 == 0))
            | ((sender == 2) & (phase < 3))
            | ((sender == 1) & (phase == 0))
        )

    def hops_here(k, m):
        if m == 2:
            return y_first(k, (role + 2) % 4)
        sender = role + 1 - 2 * (role % 2)
        return (sender != 3) & jnp.logical_not(y_first(k, sender))

    def relays_here(k, m):
        even = turn(k) % 2 == 0
        if m == 1:
            return (role >= 2) | ((role == 1) & even)
        return (role == 3) | ((role == 2) & (turn(k) % 2 == 1))

    def send_chunk(k):
        for m in (1, 2):
            col_copy(k, m).start()
        hop = y_first(k, role)

        @pl.when(hop)
        def _():
            hop_copy(k, 2).start()

        @pl.when(jnp.logical_not(hop) & (role != 3))
        def _():
            hop_copy(k, 1).start()

        for m in (1, 2):
            @pl.when(role != m)
            def _():
                row_copy(k, m).start()

    def blocks(count, send_sem, recv_sem):
        area = hop_ref.at[0, pl.ds(0, count)]
        return pltpu.make_async_remote_copy(
            src_ref=area, dst_ref=area, send_sem=send_sem, recv_sem=recv_sem,
            device_id=(peers[1], col), device_id_type=MESH)

    def sent_chunk(k):
        slot = sent.at[k % slots]

        @pl.when(role == 0)
        def _():
            blocks(5, slot, col_recv.at[0]).wait_send()

        @pl.when(role != 0)
        def _():
            blocks(4, slot, col_recv.at[0]).wait_send()

    def relay(k):
        blocks(2, sent.at[0], col_recv.at[k]).wait_recv()
        for m in (1, 2):
            @pl.when(relays_here(k, m))
            def _():
                relay_copy(k, m).start()

        first, second = hops_here(k, 1), hops_here(k, 2)

        @pl.when(first & second)
        def _():
            blocks(2, sent.at[0], h_recv.at[k]).wait_recv()

        @pl.when(first != second)
        def _():
            blocks(1, sent.at[0], h_recv.at[k]).wait_recv()

        for m, here in ((1, first), (2, second)):
            @pl.when(here)
            def _():
                hop_forward(k, m).start()

    def pass_rows(p, same):
        source = rxq.at[p] if same else rxr.at[p, :, pl.ds(0, 8 * rows)]
        return pltpu.make_async_remote_copy(
            src_ref=source, dst_ref=rxr.at[p, :, pl.ds(8 * rows, 8 * rows)],
            send_sem=m_send.at[p % PASSES], recv_sem=m_recv.at[p],
            device_id=(tok, mate), device_id_type=MESH)

    def pass_cols(p):
        return pltpu.make_async_remote_copy(
            src_ref=rxq.at[p, pl.ds((1 - core) * piece, piece)], dst_ref=rxm.at[p],
            send_sem=m_send.at[p % PASSES], recv_sem=m_recv.at[p],
            device_id=(tok, mate), device_id_type=MESH)

    def passed(p):
        return blocks(12, m_send.at[p % PASSES], m_recv.at[p])

    def arrivals(p):
        @pl.when(p >= PASSES)
        def _():
            passed(p - PASSES).wait_send()

        @pl.when(role != 0)
        def _():
            blocks(8, sent.at[0], in_recv.at[p]).wait_recv()
            pass_rows(p, False).start()

        @pl.when(role == 0)
        def _():
            blocks(2, sent.at[0], in_recv.at[p]).wait_recv()
            pass_rows(p, True).start()
            for f in range(wide):
                rxr[p, f, pl.ds(0, 8 * rows)] = rxq[p, f]

        pass_cols(p).start()

    def loads(k):
        copies = [pltpu.make_async_copy(full_ref.at[k, mate], xbuf.at[mate], load_sem.at[1])]
        for m in range(1, planes):
            other = ((plane + m) % planes) * 2
            copies.append(pltpu.make_async_copy(
                full_ref.at[k, pl.ds(other, 2)], xbuf.at[pl.ds(other, 2)], load_sem.at[1 + m]))
        return copies

    groups = 2 * planes * piece

    def rotate(k):
        slot = k % slots

        block = xbuf[...].reshape(groups * rows, LANES)
        out = jnp.dot(block, table_ref[...], preferred_element_type=jnp.float32)
        tmp[...] = out.reshape(groups, rows, LANES)

        def butterfly(index, carry):
            r = pl.multiple_of((index // (LANES // 128)) * 16, 16)
            lane = pl.multiple_of((index % (LANES // 128)) * 128, 128)
            values = [tmp[g, pl.ds(r, 16), pl.ds(lane, 128)] for g in range(groups)]
            step = 1
            while step < groups:
                values = [
                    values[g] + values[g + step] if g & step == 0 else values[g - step] - values[g]
                    for g in range(groups)
                ]
                step *= 2
            total = squares[0]
            for g in range(groups):
                rounded = (values[g] * scale).astype(jnp.bfloat16)
                rot[slot, g, pl.ds(r, 16), pl.ds(lane, 128)] = rounded
                exact = rounded.astype(jnp.float32)
                total = total + exact * exact
            squares[0] = total
            return carry

        lax.fori_loop(0, (rows // 16) * (LANES // 128), butterfly, 0)
        for f in range(wide):
            rxr[k // 2, f, place(k, 0)] = rot[slot, tok * wide + f]
            rxq[k // 2, f, place(k, 0)] = rot[slot, plane * wide + f]
        send_chunk(k)

    def row_block(k, f):
        left = rxr[k, f].T
        start = pl.multiple_of(f * LANES, LANES)
        for n in range(piece):
            right = jnp.concatenate([rxq[k, core * piece + n], rxm[k, n]], axis=0)
            out = jnp.dot(left, right, preferred_element_type=jnp.float32)
            acc[pl.ds(start, LANES), pl.ds(n * LANES, LANES)] += out

    def joined(k):
        passed(k).wait_recv()

    def gram(k):
        joined(k)

        def body(f, carry):
            row_block(k, f)
            return carry

        lax.fori_loop(0, wide, body, 0)

    def gram_keep(f):
        span = pl.ds(pl.multiple_of(f * LANES, LANES), LANES)
        return pltpu.make_async_copy(acc.at[span], gram_ref.at[span], out_sem.at[f])

    def square_copy(m):
        target = (tok, mate) if m == 4 else (peers[m % 4], col if m < 4 else mate)
        return pltpu.make_async_remote_copy(
            src_ref=squares.at[0], dst_ref=squares.at[m],
            send_sem=s_send.at[0], recv_sem=s_recv.at[0],
            device_id=target, device_id_type=MESH)

    def squares_done():
        return pltpu.make_async_remote_copy(
            src_ref=squares.at[pl.ds(1, 7)], dst_ref=squares.at[pl.ds(1, 7)],
            send_sem=s_send.at[0], recv_sem=s_recv.at[0],
            device_id=(tok, mate), device_id_type=MESH)

    fetch(0)
    fetch(1)
    turn_half(0)
    pl.semaphore_wait(barrier, len(greet))
    part_copy(0).start()
    own_sends(0)
    fetch(2)
    squares[0] = jnp.zeros((16, 128), jnp.float32)

    def clear(index, carry):
        start = pl.multiple_of(index * 64, 64)
        acc[pl.ds(start, 64)] = jnp.zeros((64, acc.shape[1]), jnp.float32)
        return carry

    lax.fori_loop(0, acc.shape[0] // 64, clear, 0)
    for distance in range(1, planes - 1):
        turn_half(distance)
        fetch(distance + 2)
        part_copy(distance).start()
        z_stage(0, distance)
        own_sends(distance)
    for k in range(planes - 1, LEAD + 1):
        turn_half(k)
        fetch(k + 2)
        part_copy(k).start()
    for k in range(planes - 1, LEAD):
        own_sends(k)

    def drain(k):
        part_copy(k).wait_send()
        for origin in range(planes):
            @pl.when(can[0] & (origin <= plane))
            def _():
                z_both(k, origin, 0).wait_send()

            @pl.when(can[1] & (origin >= plane))
            def _():
                z_both(k, origin, 1).wait_send()
        for m in (1, 2):
            @pl.when(relays_here(k, m))
            def _():
                relay_copy(k, m).wait_send()

            @pl.when(hops_here(k, m))
            def _():
                hop_forward(k, m).wait_send()

    def step(k, carry):
        z_stage(k, planes - 1)
        for copy in loads(k):
            copy.start()

        @pl.when(k + 1 < chunks)
        def _():
            z_stage(k + 1, 1)

        @pl.when(k + LEAD < chunks)
        def _():
            own_sends(k + LEAD)

        @pl.when(k + LEAD + 1 < chunks)
        def _():
            turn_half(k + LEAD + 1)
            part_copy(k + LEAD + 1).start()

        @pl.when(k + LEAD + 3 < chunks)
        def _():
            fetch(k + LEAD + 3)

        @pl.when(k >= RELAY_LAG)
        def _():
            relay(k - RELAY_LAG)

        @pl.when(k >= slots)
        def _():
            sent_chunk(k - slots)

        for copy in loads(k):
            copy.wait()
        xbuf[col] = half[core, k]
        rotate(k)

        @pl.when(k + 1 < chunks)
        def _():
            for distance in range(2, planes - 1):
                z_stage(k + 1, distance)

        @pl.when((k % 2 == 1) & (k // 2 >= LAG))
        def _():
            arrivals(k // 2 - LAG)

        @pl.when((k % 2 == 1) & (k // 2 > LAG))
        def _():
            gram(k // 2 - LAG - 1)

        @pl.when(k >= DRAIN)
        def _():
            drain(k - DRAIN)

        return carry

    lax.fori_loop(0, chunks, step, 0)
    for m in range(1, 8):
        square_copy(m).start()
    pairs = chunks // 2
    last = pairs - 1
    for k in range(chunks - RELAY_LAG, chunks):
        relay(k)

    def tail(p, carry):
        arrivals(p)
        gram(p - 1)
        for k in (0, 1):
            drain(2 * (p + LAG) - DRAIN + k)
        return carry

    lax.fori_loop(pairs - LAG, pairs, tail, 0)
    squares_done().wait()
    sums = squares[0]
    for m in range(1, 8):
        sums = sums + squares[m]
    lift = damp_ref[0] * (jnp.sum(sums) / D)
    joined(last)

    def final(f, carry):
        left = rxr[last, f].T
        start = pl.multiple_of(f * LANES, LANES)
        for n in range(piece):
            right = jnp.concatenate([rxq[last, core * piece + n], rxm[last, n]], axis=0)
            out = jnp.dot(left, right, preferred_element_type=jnp.float32)
            here = (pl.ds(start, LANES), pl.ds(n * LANES, LANES))
            acc[here] += out

            @pl.when((role == 0) & (f == core * piece + n))
            def _():
                row = lax.broadcasted_iota(jnp.int32, (LANES, LANES), 0)
                column = lax.broadcasted_iota(jnp.int32, (LANES, LANES), 1)
                acc[here] += lift * (row == column).astype(jnp.float32)

        @pl.when(f > 0)
        def _():
            gram_keep(f - 1).start()

        return carry

    lax.fori_loop(0, wide, final, 0)
    gram_keep(wide - 1).start()

    def rest(k, carry):
        @pl.when(k >= chunks - DRAIN + 2 * LAG)
        def _():
            drain(k)

        @pl.when(k >= chunks - slots)
        def _():
            sent_chunk(k)

        return carry

    lax.fori_loop(chunks - max(DRAIN, slots), chunks, rest, 0)
    for p in range(pairs - PASSES, pairs):
        passed(p).wait_send()

    def finish(f, carry):
        gram_keep(f).wait()
        return carry

    lax.fori_loop(0, wide, finish, 0)


ROWS = 16
SLOTS = 12
LEAD = 4
RELAY_LAG = 2
LAG = 3
DRAIN = 8
RING = 14
PASSES = 4


def fits(row_bank, token_ids):
    col_width, tok_rows = row_bank.shape[1], token_ids.shape[0]
    col_count, tok_count = lax.axis_size("col"), lax.axis_size("tok")
    return (
        col_width % LANES == 0
        and tok_count == 4
        and col_count == 8
        and D // tok_count == 2 * col_width
        and tok_rows % (4 * ROWS) == 0
        and tok_rows // (2 * ROWS) >= 2 * SLOTS
        and tok_rows * D * 7 // 2 + D // tok_count * col_width * 4 <= 54 * 2**20
    )


def fused(row_bank, token_ids, sign_flips, damping):
    col_width = row_bank.shape[1]
    col_count = lax.axis_size("col")
    tok_count = lax.axis_size("tok")
    tok_rows = token_ids.shape[0]
    planes = col_count // 2
    rows = ROWS
    chunks = tok_rows // 2 // rows
    piece = col_width // LANES
    wide = 2 * piece
    groups = D // LANES
    spread = LANES // BLOCK
    inner = jnp.asarray(np.kron(np.eye(spread), sylvester(BLOCK)), jnp.bfloat16)
    outer = jnp.asarray(np.kron(sylvester(spread), np.eye(BLOCK)), jnp.bfloat16)
    picked = row_bank.at[token_ids].get(
        mode="promise_in_bounds", wrap_negative_indices=False
    ).reshape(2, chunks, rows, col_width)
    any_space = pl.BlockSpec(memory_space=pl.ANY)
    vmem = pl.BlockSpec(memory_space=pltpu.VMEM)
    dma = pltpu.SemaphoreType.DMA
    height = D // tok_count
    gram, _, _ = pl.pallas_call(
        functools.partial(fused_kernel, planes, chunks, rows, piece, SLOTS, 1.0 / math.sqrt(D),
                          tok_rows * tok_count),
        out_shape=(
            jax.ShapeDtypeStruct((height, col_width), jnp.float32),
            jax.ShapeDtypeStruct((chunks, col_count, piece, rows, LANES), jnp.bfloat16),
            jax.ShapeDtypeStruct((2, chunks, wide, rows, LANES), jnp.bfloat16),
        ),
        in_specs=[any_space, vmem, pl.BlockSpec(memory_space=pltpu.SMEM), vmem, vmem],
        out_specs=(any_space, any_space, any_space),
        scratch_shapes=[
            pltpu.VMEM((2, 2, rows, col_width), jnp.bfloat16),
            pltpu.VMEM((2, chunks, piece, rows, LANES), jnp.bfloat16),
            pltpu.VMEM((col_count, piece, rows, LANES), jnp.bfloat16),
            pltpu.VMEM((groups, rows, LANES), jnp.float32),
            pltpu.VMEM((SLOTS, groups, rows, LANES), jnp.bfloat16),
            pltpu.VMEM((chunks // 2, wide, 16 * rows, LANES), jnp.bfloat16),
            pltpu.VMEM((chunks // 2, wide, 8 * rows, LANES), jnp.bfloat16),
            pltpu.VMEM((chunks // 2, piece, 8 * rows, LANES), jnp.bfloat16),
            pltpu.VMEM((height, col_width), jnp.float32),
            pltpu.VMEM((8, 16, 128), jnp.float32),
            dma((RING,)), dma((chunks,)),
            dma((RING, planes + 1)), dma((chunks, planes - 1)),
            dma((SLOTS,)), dma((chunks,)), dma((chunks // 2,)), dma((RING, 2)),
            dma((RING, 2)), dma((chunks,)),
            dma((PASSES,)), dma((chunks // 2,)),
            dma((1,)), dma((1,)),
            dma((2, 2)), dma((planes + 1,)), dma((wide,)),
        ],
        compiler_params=pltpu.CompilerParams(
            collective_id=0, has_side_effects=True, vmem_limit_bytes=67043328
        ),
    )(picked, sign_flips[None, :], damping, inner, outer)
    return gram * jnp.float32(1.0 / (tok_rows * tok_count))


def damped(gram_block, damping, mean_diag):
    block_rows, col_width = gram_block.shape
    row_index = lax.axis_index("tok") * block_rows + lax.broadcasted_iota(
        jnp.int32, gram_block.shape, 0
    )
    col_index = lax.axis_index("col") * col_width + lax.broadcasted_iota(
        jnp.int32, gram_block.shape, 1
    )
    on_diag = (row_index == col_index).astype(jnp.float32)
    return gram_block + damping[0] * mean_diag * on_diag


def plain(row_bank, token_ids, sign_flips, damping):
    col_width = row_bank.shape[1]
    col_count = lax.axis_size("col")
    tok_count = lax.axis_size("tok")
    tok_rows = token_ids.shape[0]
    groups = D // BLOCK
    scale = 1.0 / math.sqrt(D)
    inner_table = hadamard(BLOCK)
    outer_table = hadamard(groups)
    col_start = lax.axis_index("col") * col_width
    picked = jnp.take(row_bank, token_ids, axis=0) * sign_flips.astype(jnp.bfloat16)[None, :]
    shaped = picked.reshape(picked.shape[0], -1, BLOCK)
    turned = jnp.einsum("rab,bc->rac", shaped, inner_table, preferred_element_type=jnp.float32)
    half_turned = turned.astype(jnp.bfloat16).reshape(picked.shape)
    grouped = half_turned.reshape(col_count, tok_rows // col_count, col_width)
    block = lax.all_to_all(grouped, "col", split_axis=0, concat_axis=2, tiled=True)[0]
    shaped = block.reshape(block.shape[0], groups, BLOCK)
    turned = (
        jnp.einsum("rab,ac->rcb", shaped, outer_table, preferred_element_type=jnp.float32) * scale
    )
    finished = turned.astype(jnp.bfloat16).reshape(block.shape)[None]
    squares = jnp.sum(jnp.square(finished.astype(jnp.float32)))
    tokens_all = tok_rows * tok_count
    square_sum = lax.psum(squares, ("tok", "col"))
    mean_diag = square_sum / tokens_all / D
    flat = lax.all_gather(finished, "col", axis=1, tiled=True).reshape(-1, D)
    own_cols = lax.dynamic_slice_in_dim(flat, col_start, col_width, 1)
    partial_sum = lax.dot_general(
        flat, own_cols, (((0,), (0,)), ((), ())), preferred_element_type=jnp.float32
    )
    gram_block = lax.psum_scatter(partial_sum, "tok", scatter_dimension=0, tiled=True) / tokens_all
    return damped(gram_block, damping, mean_diag)


def shards(row_bank, token_ids, sign_flips, damping):
    run = fused if fits(row_bank, token_ids) else plain
    return run(row_bank, token_ids, sign_flips, damping)


def solution(mesh):
    in_specs = (P(None, "col"), P("tok"), P("col"), P())
    out_specs = P("tok", "col")
    return jax.shard_map(shards, mesh=mesh, in_specs=in_specs, out_specs=out_specs, check_vma=False)
```
